32 devices in a mesh: grp: 2 (over x), tok: 8 (over z, y), side: 2 (over core).
Axes of the slice: x: 2, y: 2, z: 4, core: 2. Of those that a mesh axis runs over, the one named last changes fastest.
Arguments:
- hidden_in: bfloat16 [512, 3072], P(('grp', 'tok')), parts along dimension 0, may hold values from -6 to 6
- queries: bfloat16 [512, 24, 128], P(('grp', 'tok'), 'side'), parts along dimension 0, may hold values from -32 to 32
- key_new: bfloat16 [512, 4, 128], P(('grp', 'tok'), 'side'), parts along dimension 0, may hold values from -32 to 32
- value_new: bfloat16 [512, 4, 128], P(('grp', 'tok'), 'side'), parts along dimension 0, may hold values from -6 to 6
- cache_keys: bfloat16 [512, 4, 128, 128], P(('grp', 'tok'), 'side'), parts along dimension 0, may hold values from -32 to 32
- cache_values: bfloat16 [512, 4, 128, 128], P(('grp', 'tok'), 'side'), parts along dimension 0, may hold values from -6 to 6
- lengths: int32 [512], P(('grp', 'tok')), parts along dimension 0, may hold values from 1 to 128, 16384 in all
- out_weight: bfloat16 [3072, 3072], P('side', 'tok'), may hold values from -0.109375 to 0.109375
- norm_gain: float32 [3072], replicated, may hold values from 0.1 to 1.9
- router_weight: float32 [3072, 4], replicated, may hold values from -0.109375 to 0.109375
- gate_weight: bfloat16 [3072, 32768], P(None, ('tok', 'side')), may hold values from -0.109375 to 0.109375
- up_weight: bfloat16 [3072, 32768], P(None, ('tok', 'side')), may hold values from -0.109375 to 0.109375
- down_weight: bfloat16 [32768, 3072], P(('tok', 'side')), may hold values from -0.0625 to 0.0625
- routes: int32 [512, 2], P('grp'), parts along dimension 0, may hold values from 0 to 3, all different within a row; in each aligned block of 32 rows (0 to 31, 32 to 63, ...) at most 24 rows name the same one
Outputs:
- mixed: bfloat16 [512, 3072], P(('grp', 'tok')), parts along dimension 0
The draws below stay inside these ranges and needn't reach their ends.
There are 2 independent parts, one for each index of `grp`. The reference program is written for one: setup_inputs(seed, part) draws one part's arguments, and reference() takes and returns one part's arrays. A program takes and returns all parts, laid end to end along the dimension named above; an argument that names none is the same for every part. Nothing has to cross between parts.
Inputs may be any that keep to these rules, and one draw needn't show every extreme that they name: Every sequence has at least one valid cache position and some sequence has 128; in each serving group the lengths sum to 16384. `routes`: each row names two different experts; among the rows of one index of tok (aligned blocks of 32 rows) no expert is named by more than 24 rows, and some expert reaches 24 in some block.
All inputs are finite; a program needn't handle non-finite values.
Results may differ from the reference program's by a relative error of at most 0.0075.
Values may be sent and summed in bfloat16 or wider, within the bound.
A program may use at most 128 MiB of HBM per device.

```python
import math
import jax
import jax.numpy as jnp
import numpy as np
from jax import lax

D = 3072
HEADS = 24
KV_HEADS = 4
HD = 128
EXPERTS = 4
HID = 8192
TOP = 2
SEQ_DEV = 32
L_MAX = 128
CAP = 24
SEQS = 256


def draw_queries(key, part):
    sampled = jnp.clip(jax.random.normal(jax.random.fold_in(key, 11), (SEQS, HEADS, HD), jnp.float32), -6.0, 6.0)
    return sampled.astype(jnp.bfloat16)


def draw_key_new(key, part):
    sampled = jnp.clip(jax.random.normal(jax.random.fold_in(key, 23), (SEQS, KV_HEADS, HD), jnp.float32), -6.0, 6.0)
    return sampled.astype(jnp.bfloat16)


def draw_cache_keys(key, part):
    sampled = jnp.clip(jax.random.normal(jax.random.fold_in(key, 37), (SEQS, KV_HEADS, L_MAX, HD), jnp.float32), -6.0, 6.0)
    return sampled.astype(jnp.bfloat16)


def steps_of(own_key, extent, pieces, least, top_value):
    factor_of, own = 1.0, jax.random.fold_in(own_key, 6)
    for dim, parts in pieces:
        heights = jnp.exp(jax.random.uniform(jax.random.fold_in(own, dim), (parts,), jnp.float32, least / len(pieces), top_value / len(pieces)))
        factor_of = factor_of * jnp.repeat(heights, extent[dim] // parts).reshape([-1 if axis == dim else 1 for axis in range(len(extent))])
    return factor_of


def profile(number_of, total, limit, slope):
    weights = [(1 << 20) // math.isqrt(standing ** slope) + 1 for standing in range(2, number_of + 1)]
    rest, counts = total - limit - (number_of - 1), [1] * (number_of - 1)
    while rest > 0:
        candidates = [i for i in range(number_of - 1) if counts[i] < limit]
        pool, budget = sum([weights[i] for i in candidates]), rest
        for i in candidates:
            extra = min(limit - counts[i], max(1, budget * weights[i] // pool), rest)
            counts[i] = counts[i] + extra
            rest = rest - extra
    return np.array([limit] + counts)


def ragged_sizes(own_key, number_of, total, most, skew):
    if number_of == 2:
        one = jax.random.randint(own_key, (), max(1, total - most), min(most, total - 1) + 1)
        return jnp.stack([one, total - one])
    sizes = jnp.asarray(profile(number_of, total, most, skew), jnp.int32)
    pairs = (number_of - 1) // 2
    source_of, taker = sizes[1:1 + 2 * pairs:2], sizes[2:2 + 2 * pairs:2]
    room = jnp.minimum(source_of - 1, most - taker)
    passed = jax.random.randint(jax.random.fold_in(own_key, 1), (pairs,), 0, 1 << 20) % (room + 1)
    sizes = sizes.at[1:1 + 2 * pairs:2].set(source_of - passed).at[2:2 + 2 * pairs:2].set(taker + passed)
    return sizes[jax.random.permutation(jax.random.fold_in(own_key, 2), number_of)]


def shared_out(own_key, own, number, rows, amount, top, bound, skew):
    ranking = jax.random.permutation(own_key, amount)
    heavy_load, usual = portions_of(amount, rows * top, bound, skew, True), portions_of(amount, rows * top, bound, skew, False)
    places = jnp.arange(amount)

    def named(sizes, turn):
        used = int((sizes > 0).sum())
        fixed = max(1, used // 4)
        moved = fixed + (places - fixed + turn * (used - fixed)) % max(1, amount - fixed)
        return jnp.zeros((amount,), jnp.int32).at[ranking[jnp.where(places < fixed, places, moved)]].set(jnp.asarray(sizes, jnp.int32))

    sizes = jnp.where(number % 4 == 0, named(heavy_load, number // 4), named(usual, number - number // 4 - 1))
    mixed = jax.random.permutation(jax.random.fold_in(own, 3), amount)
    source_of, sink = mixed[0:amount // 2 * 2:2], mixed[1:amount // 2 * 2:2]
    slack = jnp.minimum(sizes[source_of] - 1, bound - sizes[sink]) // 2
    slack = jnp.where((source_of == ranking[0]) | (sink == ranking[0]) | (sizes[sink] == 0), 0, jnp.maximum(slack, 0))
    moved = jax.random.randint(jax.random.fold_in(own, 4), (amount // 2,), 0, 1 << 20) % (slack + 1)
    sizes = sizes.at[source_of].add(-moved).at[sink].add(moved)
    labels = jnp.searchsorted(jnp.cumsum(sizes), jnp.arange(rows * top), side="right").astype(jnp.int32)
    table = labels.reshape(top, rows).T
    table = table[jax.random.permutation(jax.random.fold_in(own, 1), rows)]
    turn = jax.random.randint(jax.random.fold_in(own, 2), (rows, 1), 0, top)
    return jnp.take_along_axis(table, (jnp.arange(top)[None, :] + turn) % top, axis=1)


def portions_of(number_of, total, bound, slope, full):
    portions = [(1 << 20) // math.isqrt(standing ** slope) + 1 for standing in range(1, number_of + 1)]
    largest = bound if full else min(bound, max(-(-total // number_of), total * portions[0] // sum(portions)))
    least = 1 if total - largest >= number_of - 1 else 0
    counts, surplus = [largest] + [least] * (number_of - 1), total - largest - least * (number_of - 1)
    while surplus > 0:
        movable = [i for i in range(1, number_of) if counts[i] < largest] or [i for i in range(1, number_of) if counts[i] < bound]
        whole, budget = sum([portions[i] for i in movable]), surplus
        for i in movable:
            extra = min(bound - counts[i], max(1, budget * portions[i] // whole), surplus)
            counts[i] = counts[i] + extra
            surplus = surplus - extra
    return np.array(counts)


def noise(own_key, shape, scale, limit, cuts=(), kind=jnp.bfloat16):
    array = jax.random.normal(own_key, shape, jnp.float32) * scale
    if len(cuts) > 0:
        array = steps_of(own_key, shape, cuts, -0.22, 0.18) * array
    return jnp.clip(array, min=-limit, max=limit).astype(kind)


def setup_inputs(seed: int = 0, part: int = 0) -> dict:
    key_of = jax.random.split(jax.random.key(seed), 15)
    part_keys = jax.random.split(jax.random.fold_in(key_of[14], part), 15)
    hidden_in = noise(part_keys[0], (SEQS, D), 1.0, 6.0, ((0, 8),))
    queries = draw_queries(jax.random.fold_in(jax.random.fold_in(key_of[14], part), 71), part)
    key_new = draw_key_new(jax.random.fold_in(jax.random.fold_in(key_of[14], part), 71), part)
    value_new = noise(part_keys[3], (SEQS, KV_HEADS, HD), 1.0, 6.0, ((0, 8), (1, 2)))
    cache_keys = draw_cache_keys(jax.random.fold_in(jax.random.fold_in(key_of[14], part), 71), part)
    cache_values = noise(part_keys[5], (SEQS, KV_HEADS, L_MAX, HD), 1.0, 6.0, ((0, 8), (1, 2)))
    lengths = ragged_sizes(part_keys[6], SEQS, SEQS * L_MAX // 2, L_MAX, 2).astype(jnp.int32)
    out_weight = noise(key_of[7], (HEADS * HD, D), (HEADS * HD) ** -0.5, 0.109375, ((0, 2), (1, 8)))
    norm_gain = jnp.clip(1.0 + 0.18 * jax.random.normal(key_of[8], (D,), jnp.float32), 0.1, 1.9)
    router_weight = noise(key_of[9], (D, EXPERTS), D ** -0.5, 0.109375, (), jnp.float32)
    gate_weight = noise(key_of[10], (D, EXPERTS * HID), D ** -0.5, 0.109375, ((1, 16),))
    up_weight = noise(key_of[11], (D, EXPERTS * HID), D ** -0.5, 0.109375, ((1, 16),))
    down_weight = noise(key_of[12], (EXPERTS * HID, D), HID ** -0.5, 0.0625, ((0, 16),))
    routes_keys = jax.random.split(jax.random.fold_in(part_keys[13], 1), SEQS // SEQ_DEV)
    routes_turns = jax.random.permutation(jax.random.fold_in(part_keys[13], 3), SEQS // SEQ_DEV)
    routes = jax.vmap(lambda own, number: shared_out(jax.random.fold_in(part_keys[13], 2), own, number, SEQ_DEV, EXPERTS, TOP, CAP, 2))(routes_keys, routes_turns).reshape((SEQS, TOP))
    return dict(hidden_in=hidden_in, queries=queries, key_new=key_new, value_new=value_new, cache_keys=cache_keys, cache_values=cache_values, lengths=lengths, out_weight=out_weight, norm_gain=norm_gain, router_weight=router_weight, gate_weight=gate_weight, up_weight=up_weight, down_weight=down_weight, routes=routes)


def reference(hidden_in, queries, key_new, value_new, cache_keys, cache_values, lengths, out_weight, norm_gain, router_weight, gate_weight, up_weight, down_weight, routes):
    group_size = HEADS // KV_HEADS
    scaling = 1.0 / math.sqrt(HD)
    grouped = queries.astype(jnp.float32).reshape(SEQS, KV_HEADS, group_size, HD)
    scores = jnp.einsum('skgd,skpd->skgp', grouped, cache_keys.astype(jnp.float32)) * scaling
    usable = jnp.arange(L_MAX, dtype=jnp.int32)[None, :] < lengths[:, None]
    scores = jnp.where(usable[:, None, None, :], scores, -jnp.inf)
    own_score = jnp.einsum('skgd,skd->skg', grouped, key_new.astype(jnp.float32)) * scaling
    top_score = jnp.maximum(lax.optimization_barrier(jnp.max(scores, axis=-1)), own_score)
    weights = jnp.exp(scores - top_score[..., None])
    own_weight = jnp.exp(own_score - top_score)
    totals = lax.optimization_barrier(jnp.sum(weights, axis=-1)) + own_weight
    prob_low = (weights / totals[..., None]).astype(jnp.bfloat16)
    own_low = (own_weight / totals).astype(jnp.bfloat16)
    mixture = jnp.einsum('skgp,skpd->skgd', prob_low.astype(jnp.float32), cache_values.astype(jnp.float32))
    mixture = mixture + own_low.astype(jnp.float32)[..., None] * value_new.astype(jnp.float32)[:, :, None, :]
    attn_out = mixture.astype(jnp.bfloat16).reshape(SEQS, HEADS * HD)
    projected = jnp.dot(attn_out, out_weight, preferred_element_type=jnp.float32)
    residual = (hidden_in.astype(jnp.float32) + projected).astype(jnp.bfloat16)
    stream = residual.astype(jnp.float32)
    normed = (stream * lax.rsqrt(lax.optimization_barrier(jnp.mean(stream * stream, axis=-1, keepdims=True)) + 1e-05) * norm_gain).astype(jnp.bfloat16)
    logits = jnp.dot(normed.astype(jnp.float32), router_weight, precision=lax.Precision.HIGHEST)
    expert_ids = jnp.arange(EXPERTS, dtype=jnp.int32)
    picks = (routes[:, :, None] == expert_ids[None, None, :]).astype(jnp.float32)
    chosen_logits = lax.optimization_barrier(jnp.sum(picks * logits[:, None, :], axis=-1))
    leading = jax.nn.sigmoid(chosen_logits[:, 0] - chosen_logits[:, 1])
    gates = jnp.stack([leading, 1.0 - leading], axis=1)
    coefficient = lax.optimization_barrier(jnp.sum(gates[:, :, None] * picks, axis=1))

    def one_expert(index):
        gate_cols = lax.dynamic_slice_in_dim(gate_weight, index * HID, HID, 1)
        up_cols = lax.dynamic_slice_in_dim(up_weight, index * HID, HID, 1)
        down_rows = lax.dynamic_slice_in_dim(down_weight, index * HID, HID, 0)
        gated = jnp.dot(normed, gate_cols, preferred_element_type=jnp.float32)
        upward = jnp.dot(normed, up_cols, preferred_element_type=jnp.float32)
        active = (jax.nn.silu(gated) * upward).astype(jnp.bfloat16)
        return jnp.dot(active, down_rows, preferred_element_type=jnp.float32)
    outputs = lax.map(one_expert, expert_ids)
    combined = lax.optimization_barrier(jnp.sum(coefficient.T[:, :, None] * outputs, axis=0))
    return (stream + combined).astype(jnp.bfloat16)
```

```python
import functools
import math

import jax
import jax.numpy as jnp
from jax import lax
from jax.experimental import pallas as pl
from jax.experimental.pallas import tpu as pltpu
from jax.sharding import PartitionSpec as P

CAP = 24


def attend(queries, key_new, value_new, cache_keys, cache_values, lengths):
    seq_count, head_count, head_width = queries.shape
    kv_count = key_new.shape[1]
    places = cache_keys.shape[2]
    scaling = 1.0 / math.sqrt(head_width)
    grouped = queries.reshape(seq_count, kv_count, head_count // kv_count, head_width)
    scores = (
        jnp.einsum("skgd,skpd->skgp", grouped, cache_keys, preferred_element_type=jnp.float32)
        * scaling
    )
    usable = jnp.arange(places, dtype=jnp.int32)[None, :] < lengths[:, None]
    scores = jnp.where(usable[:, None, None, :], scores, -jnp.inf)
    own_score = (
        jnp.einsum("skgd,skd->skg", grouped, key_new, preferred_element_type=jnp.float32) * scaling
    )
    top_score = jnp.maximum(jnp.max(scores, axis=-1), own_score)
    weights = jnp.exp(scores - top_score[..., None])
    own_weight = jnp.exp(own_score - top_score)
    totals = jnp.sum(weights, axis=-1) + own_weight
    prob_low = (weights / totals[..., None]).astype(jnp.bfloat16)
    own_low = (own_weight / totals).astype(jnp.bfloat16)
    mixture = jnp.einsum(
        "skgp,skpd->skgd", prob_low, cache_values, preferred_element_type=jnp.float32
    )
    mixture = (
        mixture
        + own_low.astype(jnp.float32)[..., None] * value_new.astype(jnp.float32)[:, :, None, :]
    )
    return mixture.astype(jnp.bfloat16).reshape(seq_count, head_count * head_width)

def wire(block):
    rows, width = block.shape
    extra = rows - 16
    half = width // 2
    tail = jnp.concatenate([block[16:, :half], block[16:, half:]], axis=0)
    return jnp.concatenate([block[:16], tail], axis=1).astype(jnp.bfloat16)


def unwire(block, width):
    half = width // 2
    full = block.astype(jnp.float32)
    tail = jnp.concatenate([full[:8, width:], full[8:, width:]], axis=1)
    return jnp.concatenate([full[:, :width], tail], axis=0)


def body(
    dims,
    attn_ref,
    hidden_ref,
    routes_ref,
    routes_t_ref,
    gain_ref,
    router_ref,
    out_w_ref,
    gate_hbm,
    up_hbm,
    down_hbm,
    out_ref,
    heads,
    proj,
    proj_peer,
    cols,
    cols_in,
    stream_buf,
    tokens,
    packed,
    active,
    gate_w,
    up_w,
    down_w,
    mine,
    theirs,
    theirs_in,
    y_out,
    y_in,
    z_out,
    z_in,
    final,
    w_sem,
    ag_zs,
    ag_zr,
    ag_ys,
    ag_yr,
    tok_s,
    tok_r,
    col_s,
    col_r,
    one_s,
    one_r,
    rz_s,
    rz_r,
    ry_s,
    ry_r,
):
    T, Z, R, rows, cap = dims
    half_rows = rows // 2
    D = hidden_ref.shape[1]
    half_d = D // 2
    total = T * rows
    slots = T * cap
    part = Z * cap
    hid = gate_w.shape[1]
    tok = lax.axis_index("tok")
    side = lax.axis_index("side")
    z = tok // R
    r = tok % R
    other = 1 - side

    def zo(d):
        return (z + d) % Z

    def ro(d):
        return (r + d) % R

    def copy(src, dst, ssem, rsem, t=None, s=None):
        where = {"tok": tok if t is None else t, "side": side if s is None else s}
        return pltpu.make_async_remote_copy(
            src_ref=src,
            dst_ref=dst,
            send_sem=ssem,
            recv_sem=rsem,
            device_id=where,
            device_id_type=pl.DeviceIdType.MESH,
        )

    loads = [
        pltpu.make_async_copy(gate_hbm, gate_w, w_sem.at[0]),
        pltpu.make_async_copy(up_hbm, up_w, w_sem.at[1]),
        pltpu.make_async_copy(down_hbm, down_w, w_sem.at[2]),
    ]
    for load in loads:
        load.start()

    barrier = pltpu.get_barrier_semaphore()
    for d in range(1, T):
        pl.semaphore_signal(
            barrier,
            inc=1,
            device_id={"tok": (tok + d) % T, "side": side},
            device_id_type=pl.DeviceIdType.MESH,
        )
    pl.semaphore_signal(
        barrier, inc=1, device_id={"tok": tok, "side": other}, device_id_type=pl.DeviceIdType.MESH
    )
    pl.semaphore_wait(barrier, T)

    z_order = sorted(range(1, Z), key=lambda d: -min(d, Z - d))
    z_wait = z_order[::-1]
    pending = []

    def gather(phase, own, slot, landed):
        for d in z_order:
            c = copy(own, slot(tok), ag_zs.at[phase, d], ag_zr.at[phase, d], t=zo(d) * R + r)
            c.start()
            pending.append(c)

        def across(src, d, holder):
            for e in range(1, R):
                c = copy(
                    src, slot(holder), ag_ys.at[phase, e, d], ag_yr.at[phase, e, d], t=z * R + ro(e)
                )
                c.start()
                pending.append(c)

        across(own, 0, tok)
        for d in z_wait:
            holder = zo(Z - d) * R + r
            copy(
                slot(holder), slot(holder), ag_zs.at[phase, d], ag_zr.at[phase, d], t=zo(d) * R + r
            ).wait_recv()
            across(slot(holder), d, holder)
            landed(holder)
        for d in [0] + z_wait:
            for e in range(1, R):
                holder = zo(Z - d) * R + ro(R - e)
                copy(
                    slot(holder),
                    slot(holder),
                    ag_ys.at[phase, e, d],
                    ag_yr.at[phase, e, d],
                    t=z * R + ro(e),
                ).wait_recv()
                landed(holder)

    def head_slot(t):
        return heads.at[pl.ds(pl.multiple_of(t * rows, rows), rows)]

    heads[pl.ds(pl.multiple_of(tok * rows, rows), rows), :] = attn_ref[...]
    gather(0, attn_ref, head_slot, lambda holder: None)

    width = out_w_ref.shape[1]
    p = jnp.dot(heads[...], out_w_ref[...], preferred_element_type=jnp.float32)
    proj[...] = p.reshape(T, 2, half_rows, width)
    c = copy(proj.at[:, other], proj_peer, one_s.at[0], one_r.at[0], s=other)
    c.start()
    pending.append(c)
    c.wait_recv()
    cols[...] = (proj[:, side] + proj_peer[...]).astype(jnp.bfloat16)
    for d in range(1, T):
        t = (tok + d) % T
        c = copy(cols.at[t], cols_in.at[tok], col_s.at[d], col_r.at[d], t=t)
        c.start()
        pending.append(c)
    cols_in[tok] = cols[tok]
    for d in range(1, T):
        t = (tok + T - d) % T
        copy(cols.at[t], cols_in.at[t], col_s.at[d], col_r.at[d], t=t).wait_recv()

    my_rows = pl.multiple_of(side * half_rows, half_rows)
    projected = jnp.concatenate([cols_in[t].astype(jnp.float32) for t in range(T)], axis=1)
    low = (hidden_ref[pl.ds(my_rows, half_rows), :].astype(jnp.float32) + projected).astype(
        jnp.bfloat16
    )
    stream_buf[pl.ds(my_rows, half_rows), :] = low
    stream = low.astype(jnp.float32)
    normed = (
        stream
        * lax.rsqrt(jnp.mean(stream * stream, axis=-1, keepdims=True) + 1e-05)
        * gain_ref[...]
    ).astype(jnp.bfloat16)

    def token_slot(t, s=None):
        s = side if s is None else s
        return tokens.at[pl.ds(pl.multiple_of(t * rows + s * half_rows, half_rows), half_rows)]

    tokens[pl.ds(pl.multiple_of(tok * rows + side * half_rows, half_rows), half_rows), :] = normed

    def over(holder):
        c = copy(
            token_slot(holder), token_slot(holder), tok_s.at[holder], tok_r.at[holder], s=other
        )
        c.start()
        pending.append(c)

    expert = z
    lanes = lax.broadcasted_iota(jnp.int32, (1, total), 1)
    block = lax.div(lanes, rows)
    hit = (routes_t_ref[0:1, :] == expert) | (routes_t_ref[1:2, :] == expert)
    row_i = lax.broadcasted_iota(jnp.int32, (total, total), 0)
    col_i = lax.broadcasted_iota(jnp.int32, (total, total), 1)
    before = (row_i < col_i) & (lax.div(row_i, rows) == lax.div(col_i, rows))
    hits = jnp.broadcast_to(jnp.where(hit, 1.0, 0.0), (8, total)).astype(jnp.bfloat16)
    rank = jnp.dot(
        hits,
        jnp.where(before, 1.0, 0.0).astype(jnp.bfloat16),
        preferred_element_type=jnp.float32,
    )[0:1].astype(jnp.int32)
    base = (lax.rem(block, R) * Z + lax.div(block, R)) * cap
    place = jnp.where(hit & (rank < cap), base + rank, -1)
    slot_i = lax.broadcasted_iota(jnp.int32, (slots, total), 0)
    put = jnp.where(slot_i == place, 1.0, 0.0).astype(jnp.bfloat16)

    over(tok)
    c = copy(
        stream_buf.at[pl.ds(my_rows, half_rows)],
        stream_buf.at[pl.ds(my_rows, half_rows)],
        one_s.at[1],
        one_r.at[1],
        s=other,
    )
    c.start()
    pending.append(c)
    gather(1, token_slot(tok), token_slot, over)
    for t in range(T):
        copy(
            token_slot(t, other), token_slot(t, other), tok_s.at[t], tok_r.at[t], s=other
        ).wait_recv()

    @pl.loop(0, D // 512)
    def _(i):
        here = pl.ds(pl.multiple_of(i * 512, 512), 512)
        packed[:, here] = jnp.dot(
            put, tokens[:, here], preferred_element_type=jnp.float32
        ).astype(jnp.bfloat16)

    loads[0].wait()
    loads[1].wait()

    @pl.loop(0, hid // 256)
    def _(i):
        here = pl.ds(pl.multiple_of(i * 256, 256), 256)
        g = jnp.dot(packed[...], gate_w[:, here], preferred_element_type=jnp.float32)
        u = jnp.dot(packed[...], up_w[:, here], preferred_element_type=jnp.float32)
        active[:, here] = (g / (1.0 + jnp.exp(-g)) * u).astype(jnp.bfloat16)

    loads[2].wait()

    @pl.loop(0, half_d // 256)
    def _(i):
        here = pl.ds(pl.multiple_of(i * 256, 256), 256)
        there = pl.ds(pl.multiple_of(other * half_d + i * 256, 256), 256)
        theirs[:, here] = jnp.dot(
            active[...], down_w[:, there], preferred_element_type=jnp.float32
        ).astype(jnp.bfloat16)

    d2d = copy(theirs, theirs_in, one_s.at[2], one_r.at[2], s=other)
    d2d.start()
    pending.append(d2d)

    @pl.loop(0, half_d // 256)
    def _(i):
        here = pl.ds(pl.multiple_of(i * 256, 256), 256)
        there = pl.ds(pl.multiple_of(side * half_d + i * 256, 256), 256)
        mine[:, here] = jnp.dot(active[...], down_w[:, there], preferred_element_type=jnp.float32)

    d2d.wait_recv()
    mine[...] = mine[...] + theirs_in[...].astype(jnp.float32)

    back = z_order + [0]
    for d in back:
        for e in range(1, R):
            at = pl.multiple_of(ro(e) * part + zo(d) * cap, 8)
            y_out[e, d] = wire(mine[pl.ds(at, cap), :])
            c = copy(y_out.at[e, d], y_in.at[e, d], ry_s.at[e, d], ry_r.at[e, d], t=z * R + ro(e))
            c.start()
            pending.append(c)
    for d in back:
        at = pl.multiple_of(r * part + zo(d) * cap, 8)
        total_rows = mine[pl.ds(at, cap), :]
        for e in range(1, R):
            copy(
                y_out.at[e, d], y_in.at[e, d], ry_s.at[e, d], ry_r.at[e, d], t=z * R + ro(e)
            ).wait_recv()
            total_rows = total_rows + unwire(y_in[e, d], half_d)
        if d == 0:
            z_in[z] = wire(total_rows)
        else:
            z_out[d] = wire(total_rows)
            c = copy(z_out.at[d], z_in.at[z], rz_s.at[d], rz_r.at[d], t=zo(d) * R + r)
            c.start()
            pending.append(c)

    own = pl.ds(pl.multiple_of(tok * rows, rows), rows)
    logits = jnp.dot(tokens[own, :], router_ref[...], preferred_element_type=jnp.float32)
    chosen = routes_ref[own, :]
    r0, r1 = chosen[:, 0:1], chosen[:, 1:2]
    lane = lax.broadcasted_iota(jnp.int32, (rows, 128), 1)

    def parts(k):
        return (lane == k) | (lane == k + Z) | (lane == k + 2 * Z)

    l0 = jnp.sum(jnp.where(parts(r0), logits, 0.0), axis=1, keepdims=True)
    l1 = jnp.sum(jnp.where(parts(r1), logits, 0.0), axis=1, keepdims=True)
    g0 = 1.0 / (1.0 + jnp.exp(l1 - l0))
    g1 = 1.0 - g0
    both = jnp.where((lane == r0) | (lane == r1), 1.0, 0.0).astype(jnp.bfloat16)
    row_n = lax.broadcasted_iota(jnp.int32, (rows, rows), 0)
    col_n = lax.broadcasted_iota(jnp.int32, (rows, rows), 1)
    ranks = jnp.dot(
        jnp.where(col_n < row_n, 1.0, 0.0).astype(jnp.bfloat16),
        both,
        preferred_element_type=jnp.float32,
    ).astype(jnp.int32)
    at = lax.broadcasted_iota(jnp.int32, (rows, part), 1)

    def find(k):
        rank = jnp.sum(jnp.where(lane == k, ranks, 0), axis=1, keepdims=True)
        return jnp.where(at == k * cap + rank, 1.0, 0.0).astype(jnp.bfloat16)

    pick0, pick1 = find(r0), find(r1)

    copy(
        stream_buf.at[pl.ds(my_rows, half_rows)],
        stream_buf.at[pl.ds(pl.multiple_of(other * half_rows, half_rows), half_rows)],
        one_s.at[1],
        one_r.at[1],
        s=other,
    ).wait_recv()
    for d in z_wait:
        src = zo(Z - d)
        copy(z_out.at[d], z_in.at[src], rz_s.at[d], rz_r.at[d], t=zo(d) * R + r).wait_recv()
    got = jnp.concatenate([unwire(z_in[e], half_d) for e in range(Z)], axis=0).astype(jnp.bfloat16)
    half = pl.ds(pl.multiple_of(side * half_d, half_d), half_d)
    mixed = (
        stream_buf[:, half].astype(jnp.float32)
        + g0 * jnp.dot(pick0, got, preferred_element_type=jnp.float32)
        + g1 * jnp.dot(pick1, got, preferred_element_type=jnp.float32)
    )
    final[side] = mixed.astype(jnp.bfloat16)
    c = copy(final.at[side], final.at[side], one_s.at[3], one_r.at[3], s=other)
    c.start()
    pending.append(c)
    copy(final.at[other], final.at[other], one_s.at[3], one_r.at[3], s=other).wait_recv()
    out_ref[:, :half_d] = final[0]
    out_ref[:, half_d:] = final[1]
    for c in pending:
        c.wait_send()


def local(
    hidden_in,
    queries,
    key_new,
    value_new,
    cache_keys,
    cache_values,
    lengths,
    out_weight,
    norm_gain,
    router_weight,
    gate_weight,
    up_weight,
    down_weight,
    routes,
):
    rows, D = hidden_in.shape
    T = lax.axis_size("tok")
    Z = router_weight.shape[1]
    R = T // Z
    cap = min(CAP, rows)
    hid = gate_weight.shape[1]
    width = out_weight.shape[1]
    bf, f32 = jnp.bfloat16, jnp.float32
    attn_out = attend(queries, key_new, value_new, cache_keys, cache_values, lengths)
    first = lax.reduce_precision(router_weight, 8, 7)
    second = lax.reduce_precision(router_weight - first, 8, 7)
    third = router_weight - first - second
    router = jnp.concatenate(
        [first, second, third, jnp.zeros((D, 128 - 3 * Z), f32)], axis=1
    ).astype(bf)
    half_d = D // 2
    wire_width = half_d * cap // 16
    dma = pltpu.SemaphoreType.DMA
    vmem = pl.BlockSpec(memory_space=pltpu.VMEM)
    anyspace = pl.BlockSpec(memory_space=pl.ANY)
    return pl.pallas_call(
        functools.partial(body, (T, Z, R, rows, cap)),
        out_shape=jax.ShapeDtypeStruct((rows, D), bf),
        in_specs=[vmem] * 7 + [anyspace] * 3,
        out_specs=vmem,
        scratch_shapes=[
            pltpu.VMEM((T * rows, attn_out.shape[1]), bf),
            pltpu.VMEM((T, 2, rows // 2, width), f32),
            pltpu.VMEM((T, rows // 2, width), f32),
            pltpu.VMEM((T, rows // 2, width), bf),
            pltpu.VMEM((T, rows // 2, width), bf),
            pltpu.VMEM((rows, D), bf),
            pltpu.VMEM((T * rows, D), bf),
            pltpu.VMEM((T * cap, D), bf),
            pltpu.VMEM((T * cap, hid), bf),
            pltpu.VMEM(gate_weight.shape, bf),
            pltpu.VMEM(up_weight.shape, bf),
            pltpu.VMEM(down_weight.shape, bf),
            pltpu.VMEM((T * cap, half_d), f32),
            pltpu.VMEM((T * cap, half_d), bf),
            pltpu.VMEM((T * cap, half_d), bf),
            pltpu.VMEM((R, Z, 16, wire_width), bf),
            pltpu.VMEM((R, Z, 16, wire_width), bf),
            pltpu.VMEM((Z, 16, wire_width), bf),
            pltpu.VMEM((Z, 16, wire_width), bf),
            pltpu.VMEM((2, rows, half_d), bf),
            dma((3,)),
            dma((2, Z)),
            dma((2, Z)),
            dma((2, R, Z)),
            dma((2, R, Z)),
            dma((T,)),
            dma((T,)),
            dma((T,)),
            dma((T,)),
            dma((4,)),
            dma((4,)),
            dma((Z,)),
            dma((Z,)),
            dma((R, Z)),
            dma((R, Z)),
        ],
        compiler_params=pltpu.CompilerParams(
            collective_id=0, has_side_effects=True, vmem_limit_bytes=67043328
        ),
    )(
        attn_out,
        hidden_in,
        routes,
        routes.T,
        norm_gain.reshape(1, D),
        router,
        out_weight,
        gate_weight,
        up_weight,
        down_weight,
    )


def solution(mesh):
    return jax.shard_map(
        local,
        mesh=mesh,
        in_specs=(
            P(("grp", "tok"), None),
            P(("grp", "tok"), "side", None),
            P(("grp", "tok"), "side", None),
            P(("grp", "tok"), "side", None),
            P(("grp", "tok"), "side", None, None),
            P(("grp", "tok"), "side", None, None),
            P(("grp", "tok")),
            P("side", "tok"),
            P(),
            P(),
            P(None, ("tok", "side")),
            P(None, ("tok", "side")),
            P(("tok", "side"), None),
            P("grp", None),
        ),
        out_specs=P(("grp", "tok"), None),
        check_vma=False,
    )
```

```python
import functools
import math

import jax
import jax.numpy as jnp
from jax import lax
from jax.experimental import pallas as pl
from jax.experimental.pallas import tpu as pltpu
from jax.sharding import PartitionSpec as P

CAP = 24
PIECES = 4
HIDDEN_TILE = 512
STRIPS = 2


def attend(queries, key_new, value_new, cache_keys, cache_values, lengths):
    seq_count, head_count, head_width = queries.shape
    kv_count = key_new.shape[1]
    places = cache_keys.shape[2]
    scaling = 1.0 / math.sqrt(head_width)
    grouped = queries.reshape(seq_count, kv_count, head_count // kv_count, head_width)
    scores = (
        jnp.einsum("skgd,skpd->skgp", grouped, cache_keys, preferred_element_type=jnp.float32)
        * scaling
    )
    usable = jnp.arange(places, dtype=jnp.int32)[None, :] < lengths[:, None]
    scores = jnp.where(usable[:, None, None, :], scores, -jnp.inf)
    own_score = (
        jnp.einsum("skgd,skd->skg", grouped, key_new, preferred_element_type=jnp.float32) * scaling
    )
    top_score = jnp.maximum(jnp.max(scores, axis=-1), own_score)
    weights = jnp.exp(scores - top_score[..., None])
    own_weight = jnp.exp(own_score - top_score)
    totals = jnp.sum(weights, axis=-1) + own_weight
    prob_low = (weights / totals[..., None]).astype(jnp.bfloat16)
    own_low = (own_weight / totals).astype(jnp.bfloat16)
    mixture = jnp.einsum(
        "skgp,skpd->skgd", prob_low, cache_values, preferred_element_type=jnp.float32
    )
    mixture = (
        mixture
        + own_low.astype(jnp.float32)[..., None] * value_new.astype(jnp.float32)[:, :, None, :]
    )
    return mixture.astype(jnp.bfloat16).reshape(seq_count, head_count * head_width)

def wire(block):
    rows, width = block.shape
    extra = rows - 16
    half = width // 2
    tail = jnp.concatenate([block[16:, :half], block[16:, half:]], axis=0)
    return jnp.concatenate([block[:16], tail], axis=1).astype(jnp.bfloat16)


def unwire(block, width):
    half = width // 2
    full = block.astype(jnp.float32)
    tail = jnp.concatenate([full[:8, width:], full[8:, width:]], axis=1)
    return jnp.concatenate([full[:, :width], tail], axis=0)


def body(
    dims,
    attn_ref,
    hidden_ref,
    routes_t_ref,
    gain_ref,
    router_ref,
    out_hbm,
    gate_hbm,
    up_hbm,
    down_hbm,
    out_ref,
    heads,
    proj,
    proj_peer,
    cols,
    cols_in,
    stream_buf,
    tokens,
    packed,
    active,
    out_w,
    gate_w,
    up_w,
    down_w,
    mine,
    theirs,
    theirs_in,
    y_out,
    y_in,
    z_out,
    z_in,
    final,
    w_sem,
    ag_zs,
    ag_zr,
    ag_ys,
    ag_yr,
    tok_s,
    tok_r,
    col_s,
    col_r,
    one_s,
    one_r,
    rz_s,
    rz_r,
    ry_s,
    ry_r,
):
    T, Z, R, rows, cap = dims
    half_rows = rows // 2
    D = hidden_ref.shape[1]
    half_d = D // 2
    total = T * rows
    slots = T * cap
    part = Z * cap
    hid = gate_w.shape[1]
    tok = lax.axis_index("tok")
    side = lax.axis_index("side")
    z = tok // R
    r = tok % R
    other = 1 - side

    def zo(d):
        return (z + d) % Z

    def ro(d):
        return (r + d) % R

    def copy(src, dst, ssem, rsem, t=None, s=None):
        where = {"tok": tok if t is None else t, "side": side if s is None else s}
        return pltpu.make_async_remote_copy(
            src_ref=src,
            dst_ref=dst,
            send_sem=ssem,
            recv_sem=rsem,
            device_id=where,
            device_id_type=pl.DeviceIdType.MESH,
        )

    loads = [
        pltpu.make_async_copy(out_hbm, out_w, w_sem.at[3]),
        pltpu.make_async_copy(gate_hbm, gate_w, w_sem.at[0]),
        pltpu.make_async_copy(up_hbm, up_w, w_sem.at[1]),
        pltpu.make_async_copy(down_hbm, down_w, w_sem.at[2]),
    ]
    for load in loads:
        load.start()

    heads[pl.ds(pl.multiple_of(tok * rows, rows), rows), :] = attn_ref[...]
    barrier = pltpu.get_barrier_semaphore()
    for d in range(1, T):
        pl.semaphore_signal(
            barrier,
            inc=1,
            device_id={"tok": (tok + d) % T, "side": side},
            device_id_type=pl.DeviceIdType.MESH,
        )
    pl.semaphore_signal(
        barrier, inc=1, device_id={"tok": tok, "side": other}, device_id_type=pl.DeviceIdType.MESH
    )
    pl.semaphore_wait(barrier, T)

    pending = []

    def gather(phase, slot, landed):
        def along(zs, hop, way, piece):
            k = (phase, hop, (way + 1) // 2, piece)
            here = slot(zs * R + r, piece)
            return copy(here, here, ag_zs.at[k], ag_zr.at[k], t=(z + way) * R + r)

        def landing(zs, hop, way, piece):
            k = (phase, hop, (way + 1) // 2, piece)
            here = slot(zs * R + r, piece)
            return copy(here, here, ag_zs.at[k], ag_zr.at[k], t=tok)

        def across(zs, piece):
            for e in range(1, R):
                k = (phase, e, zs, piece)
                here = slot(zs * R + r, piece)
                c = copy(here, here, ag_ys.at[k], ag_yr.at[k], t=z * R + ro(e))
                c.start()

        def crossed(zs, piece):
            for e in range(1, R):
                k = (phase, e, zs, piece)
                here = slot(zs * R + ro(R - e), piece)
                copy(here, here, ag_ys.at[k], ag_yr.at[k], t=z * R + ro(e)).wait_recv()
                landed(zs * R + ro(R - e), piece)

        def send_on(zs, hop, way, piece):
            ok = (z + way >= 0) & (z + way < Z)

            @pl.when(ok)
            def _():
                along(zs, hop, way, piece).start()

        for piece in range(PIECES):
            for way in (1, -1):
                send_on(z, 0, way, piece)
            across(z, piece)
        for hop in range(1, Z):
            for piece in range(PIECES):
                for way in (1, -1):
                    zs = z - way * hop

                    @pl.when((zs >= 0) & (zs < Z))
                    def _(zs=zs, way=way, piece=piece, hop=hop):
                        landing(zs, hop - 1, way, piece).wait_recv()
                        if hop < Z - 1:
                            send_on(zs, hop, way, piece)
                        across(zs, piece)
                        landed(zs * R + r, piece)

            for piece in range(PIECES):
                if hop == 1:
                    crossed(z, piece)
                else:
                    for way in (1, -1):
                        zs = z - way * (hop - 1)

                        @pl.when((zs >= 0) & (zs < Z))
                        def _(zs=zs, piece=piece):
                            crossed(zs, piece)

        for piece in range(PIECES):
            for way in (1, -1):
                zs = z - way * (Z - 1)

                @pl.when((zs >= 0) & (zs < Z))
                def _(zs=zs, piece=piece):
                    crossed(zs, piece)

    def settle(phase, slot):
        for piece in range(PIECES):
            for zs in range(Z):
                for e in range(1, R):
                    k = (phase, e, zs, piece)
                    here = slot(zs * R + r, piece)
                    copy(here, here, ag_ys.at[k], ag_yr.at[k], t=z * R + ro(e)).wait_send()
            for hop in range(Z - 1):
                for way in (1, -1):
                    zs = z - way * hop
                    ok = (zs >= 0) & (zs < Z) & (z + way >= 0) & (z + way < Z)

                    @pl.when(ok)
                    def _(zs=zs, hop=hop, way=way, piece=piece):
                        k = (phase, hop, (way + 1) // 2, piece)
                        here = slot(zs * R + r, piece)
                        copy(
                            here, here, ag_zs.at[k], ag_zr.at[k], t=(z + way) * R + r
                        ).wait_send()

    head_piece = heads.shape[1] // PIECES

    def head_slot(t, piece):
        return heads.at[
            pl.ds(pl.multiple_of(t * rows, rows), rows), pl.ds(piece * head_piece, head_piece)
        ]

    gather(0, head_slot, lambda holder, piece: None)
    loads[0].wait()

    width = out_w.shape[1]
    p = jnp.dot(heads[...], out_w[...], preferred_element_type=jnp.float32)
    proj[...] = p.reshape(T, 2, half_rows, width)
    c = copy(proj.at[:, other], proj_peer, one_s.at[0], one_r.at[0], s=other)
    c.start()
    pending.append(c)
    c.wait_recv()
    cols[...] = (proj[:, side] + proj_peer[...]).astype(jnp.bfloat16)
    for d in range(1, T):
        t = (tok + d) % T
        c = copy(cols.at[t], cols_in.at[tok], col_s.at[d], col_r.at[d], t=t)
        c.start()
        pending.append(c)
    cols_in[tok] = cols[tok]
    for d in range(1, T):
        t = (tok + T - d) % T
        copy(cols.at[t], cols_in.at[t], col_s.at[d], col_r.at[d], t=t).wait_recv()

    my_rows = pl.multiple_of(side * half_rows, half_rows)
    projected = jnp.concatenate([cols_in[t].astype(jnp.float32) for t in range(T)], axis=1)
    low = (hidden_ref[pl.ds(my_rows, half_rows), :].astype(jnp.float32) + projected).astype(
        jnp.bfloat16
    )
    stream_buf[pl.ds(my_rows, half_rows), :] = low
    stream = low.astype(jnp.float32)
    normed = (
        stream
        * lax.rsqrt(jnp.mean(stream * stream, axis=-1, keepdims=True) + 1e-05)
        * gain_ref[...]
    ).astype(jnp.bfloat16)

    token_piece = D // PIECES

    def token_slot(t, piece, s=None):
        s = side if s is None else s
        return tokens.at[
            pl.ds(pl.multiple_of(t * rows + s * half_rows, half_rows), half_rows),
            pl.ds(piece * token_piece, token_piece),
        ]

    tokens[pl.ds(pl.multiple_of(tok * rows + side * half_rows, half_rows), half_rows), :] = normed

    def over(holder, piece, s=None):
        here = token_slot(holder, piece, s)
        return copy(here, here, tok_s.at[holder, piece], tok_r.at[holder, piece], s=other)

    expert = z
    lanes = lax.broadcasted_iota(jnp.int32, (1, total), 1)
    block = lax.div(lanes, rows)
    hit = (routes_t_ref[0:1, :] == expert) | (routes_t_ref[1:2, :] == expert)
    row_i = lax.broadcasted_iota(jnp.int32, (total, total), 0)
    col_i = lax.broadcasted_iota(jnp.int32, (total, total), 1)
    before = (row_i < col_i) & (lax.div(row_i, rows) == lax.div(col_i, rows))
    hits = jnp.broadcast_to(jnp.where(hit, 1.0, 0.0), (8, total)).astype(jnp.bfloat16)
    rank = jnp.dot(
        hits,
        jnp.where(before, 1.0, 0.0).astype(jnp.bfloat16),
        preferred_element_type=jnp.float32,
    )[0:1].astype(jnp.int32)
    base = (lax.rem(block, R) * Z + lax.div(block, R)) * cap
    place = jnp.where(hit & (rank < cap), base + rank, -1)
    slot_i = lax.broadcasted_iota(jnp.int32, (slots, total), 0)
    put = jnp.where(slot_i == place, 1.0, 0.0).astype(jnp.bfloat16)

    for piece in range(PIECES):
        over(tok, piece).start()
    c = copy(
        stream_buf.at[pl.ds(my_rows, half_rows)],
        stream_buf.at[pl.ds(my_rows, half_rows)],
        one_s.at[1],
        one_r.at[1],
        s=other,
    )
    c.start()
    pending.append(c)
    gather(1, token_slot, lambda holder, piece: over(holder, piece).start())
    for t in range(T):
        for piece in range(PIECES):
            over(t, piece, other).wait_recv()

    @pl.loop(0, D // 512)
    def _(i):
        here = pl.ds(pl.multiple_of(i * 512, 512), 512)
        packed[:, here] = jnp.dot(
            put, tokens[:, here], preferred_element_type=jnp.float32
        ).astype(jnp.bfloat16)

    loads[1].wait()
    loads[2].wait()

    tile = min(HIDDEN_TILE, hid)

    @pl.loop(0, hid // tile)
    def _(i):
        here = pl.ds(pl.multiple_of(i * tile, tile), tile)
        g = jnp.dot(packed[...], gate_w[:, here], preferred_element_type=jnp.float32)
        u = jnp.dot(packed[...], up_w[:, here], preferred_element_type=jnp.float32)
        active[:, here] = (g / (1.0 + jnp.exp(-g)) * u).astype(jnp.bfloat16)

    loads[3].wait()

    strip = half_d // STRIPS
    far_up = z < Z // 2

    def down(start, q):
        at = pl.ds(pl.multiple_of(start * half_d + q * strip, 128), strip)
        return jnp.dot(active[...], down_w[:, at], preferred_element_type=jnp.float32)

    def y_copy(q, e, k):
        i = (q, e, k)
        return copy(y_out.at[i], y_in.at[i], ry_s.at[i], ry_r.at[i], t=z * R + ro(e))

    def cores_copy(q):
        return copy(theirs.at[q], theirs_in.at[q], one_s.at[q + 4], one_r.at[q + 4], s=other)

    for q in range(STRIPS):
        theirs[q] = down(other, q).astype(jnp.bfloat16)
        cores_copy(q).start()
        mine[q] = down(side, q)
        cores_copy(q).wait_recv()
        mine[q] = mine[q] + theirs_in[q].astype(jnp.float32)
        for k in range(Z):
            to = jnp.where(far_up, Z - 1 - k, k)
            for e in range(1, R):
                at = pl.multiple_of(ro(e) * part + to * cap, 8)
                y_out[q, e, k] = wire(mine[q, pl.ds(at, cap), :])
                y_copy(q, e, k).start()
    for q in range(STRIPS):
        for k in range(Z):
            to = jnp.where(far_up, Z - 1 - k, k)
            at = pl.multiple_of(r * part + to * cap, 8)
            total_rows = mine[q, pl.ds(at, cap), :]
            for e in range(1, R):
                y_copy(q, e, k).wait_recv()
                total_rows = total_rows + unwire(y_in[q, e, k], strip)
            z_out[q, to] = wire(total_rows)

            @pl.when(to == z)
            def _(to=to, q=q):
                z_in[q, z] = z_out[q, to]

            @pl.when(to != z)
            def _(to=to, q=q):
                copy(
                    z_out.at[q, to], z_in.at[q, z], rz_s.at[q, to], rz_r.at[q, z], t=to * R + r
                ).start()

    own = pl.ds(pl.multiple_of(tok * rows, rows), rows)
    mine_now = tokens[own, :].astype(jnp.float32)
    lane_t = lax.broadcasted_iota(jnp.int32, (rows, total), 1)
    row_t = lax.broadcasted_iota(jnp.int32, (rows, total), 0)
    at_own = lane_t == tok * rows + row_t

    def own_route(k):
        return jnp.sum(jnp.where(at_own, routes_t_ref[k : k + 1, :], 0), axis=1, keepdims=True)

    r0, r1 = own_route(0), own_route(1)
    lane = lax.broadcasted_iota(jnp.int32, (rows, 128), 1)
    l0 = jnp.zeros((rows, 1), jnp.float32)
    l1 = jnp.zeros((rows, 1), jnp.float32)
    for k in range(Z):
        logit = jnp.sum(mine_now * router_ref[k : k + 1, :], axis=1, keepdims=True)
        l0 = jnp.where(r0 == k, logit, l0)
        l1 = jnp.where(r1 == k, logit, l1)
    g0 = 1.0 / (1.0 + jnp.exp(l1 - l0))
    g1 = 1.0 - g0
    both = jnp.where((lane == r0) | (lane == r1), 1.0, 0.0).astype(jnp.bfloat16)
    row_n = lax.broadcasted_iota(jnp.int32, (rows, rows), 0)
    col_n = lax.broadcasted_iota(jnp.int32, (rows, rows), 1)
    ranks = jnp.dot(
        jnp.where(col_n < row_n, 1.0, 0.0).astype(jnp.bfloat16),
        both,
        preferred_element_type=jnp.float32,
    ).astype(jnp.int32)
    at = lax.broadcasted_iota(jnp.int32, (rows, part), 1)

    def find(k):
        rank = jnp.sum(jnp.where(lane == k, ranks, 0), axis=1, keepdims=True)
        return jnp.where(at == k * cap + rank, 1.0, 0.0).astype(jnp.bfloat16)

    pick0, pick1 = find(r0), find(r1)

    copy(
        stream_buf.at[pl.ds(my_rows, half_rows)],
        stream_buf.at[pl.ds(pl.multiple_of(other * half_rows, half_rows), half_rows)],
        one_s.at[1],
        one_r.at[1],
        s=other,
    ).wait_recv()
    strips = []
    for q in range(STRIPS):
        for d in range(1, Z):
            src = zo(d)
            here = z_in.at[q, src]
            copy(here, here, rz_s.at[q, src], rz_r.at[q, src], t=src * R + r).wait_recv()
        got = jnp.concatenate([unwire(z_in[q, e], strip) for e in range(Z)], axis=0)
        got = got.astype(jnp.bfloat16)
        strips.append(
            g0 * jnp.dot(pick0, got, preferred_element_type=jnp.float32)
            + g1 * jnp.dot(pick1, got, preferred_element_type=jnp.float32)
        )
    half = pl.ds(pl.multiple_of(side * half_d, half_d), half_d)
    mixed = stream_buf[:, half].astype(jnp.float32) + jnp.concatenate(strips, axis=1)
    final[side] = mixed.astype(jnp.bfloat16)
    c = copy(final.at[side], final.at[side], one_s.at[3], one_r.at[3], s=other)
    c.start()
    pending.append(c)
    copy(final.at[other], final.at[other], one_s.at[3], one_r.at[3], s=other).wait_recv()
    out_ref[:, :half_d] = final[0]
    out_ref[:, half_d:] = final[1]
    for c in pending:
        c.wait_send()
    for q in range(STRIPS):
        cores_copy(q).wait_send()
        for e in range(1, R):
            for k in range(Z):
                y_copy(q, e, k).wait_send()
        for d in range(1, Z):
            to = zo(d)
            copy(
                z_out.at[q, to], z_in.at[q, z], rz_s.at[q, to], rz_r.at[q, z], t=to * R + r
            ).wait_send()
    settle(0, head_slot)
    settle(1, token_slot)
    for t in range(T):
        for piece in range(PIECES):
            over(t, piece).wait_send()


def local(
    hidden_in,
    queries,
    key_new,
    value_new,
    cache_keys,
    cache_values,
    lengths,
    out_weight,
    norm_gain,
    router_weight,
    gate_weight,
    up_weight,
    down_weight,
    routes,
):
    rows, D = hidden_in.shape
    T = lax.axis_size("tok")
    Z = router_weight.shape[1]
    R = T // Z
    cap = min(CAP, rows)
    hid = gate_weight.shape[1]
    width = out_weight.shape[1]
    bf, f32 = jnp.bfloat16, jnp.float32
    attn_out = attend(queries, key_new, value_new, cache_keys, cache_values, lengths)
    half_d = D // 2
    strip = half_d // STRIPS
    wire_width = strip * cap // 16
    dma = pltpu.SemaphoreType.DMA
    vmem = pl.BlockSpec(memory_space=pltpu.VMEM)
    anyspace = pl.BlockSpec(memory_space=pl.ANY)
    return pl.pallas_call(
        functools.partial(body, (T, Z, R, rows, cap)),
        out_shape=jax.ShapeDtypeStruct((rows, D), bf),
        in_specs=[vmem] * 5 + [anyspace] * 4,
        out_specs=vmem,
        scratch_shapes=[
            pltpu.VMEM((T * rows, attn_out.shape[1]), bf),
            pltpu.VMEM((T, 2, rows // 2, width), f32),
            pltpu.VMEM((T, rows // 2, width), f32),
            pltpu.VMEM((T, rows // 2, width), bf),
            pltpu.VMEM((T, rows // 2, width), bf),
            pltpu.VMEM((rows, D), bf),
            pltpu.VMEM((T * rows, D), bf),
            pltpu.VMEM((T * cap, D), bf),
            pltpu.VMEM((T * cap, hid), bf),
            pltpu.VMEM(out_weight.shape, bf),
            pltpu.VMEM(gate_weight.shape, bf),
            pltpu.VMEM(up_weight.shape, bf),
            pltpu.VMEM(down_weight.shape, bf),
            pltpu.VMEM((STRIPS, T * cap, strip), f32),
            pltpu.VMEM((STRIPS, T * cap, strip), bf),
            pltpu.VMEM((STRIPS, T * cap, strip), bf),
            pltpu.VMEM((STRIPS, R, Z, 16, wire_width), bf),
            pltpu.VMEM((STRIPS, R, Z, 16, wire_width), bf),
            pltpu.VMEM((STRIPS, Z, 16, wire_width), bf),
            pltpu.VMEM((STRIPS, Z, 16, wire_width), bf),
            pltpu.VMEM((2, rows, half_d), bf),
            dma((4,)),
            dma((2, Z - 1, 2, PIECES)),
            dma((2, Z - 1, 2, PIECES)),
            dma((2, R, Z, PIECES)),
            dma((2, R, Z, PIECES)),
            dma((T, PIECES)),
            dma((T, PIECES)),
            dma((T,)),
            dma((T,)),
            dma((4 + STRIPS,)),
            dma((4 + STRIPS,)),
            dma((STRIPS, Z)),
            dma((STRIPS, Z)),
            dma((STRIPS, R, Z)),
            dma((STRIPS, R, Z)),
        ],
        compiler_params=pltpu.CompilerParams(
            collective_id=0, has_side_effects=True, vmem_limit_bytes=67043328
        ),
    )(
        attn_out,
        hidden_in,
        routes.T,
        norm_gain.reshape(1, D),
        router_weight.T,
        out_weight,
        gate_weight,
        up_weight,
        down_weight,
    )


def solution(mesh):
    return jax.shard_map(
        local,
        mesh=mesh,
        in_specs=(
            P(("grp", "tok"), None),
            P(("grp", "tok"), "side", None),
            P(("grp", "tok"), "side", None),
            P(("grp", "tok"), "side", None),
            P(("grp", "tok"), "side", None, None),
            P(("grp", "tok"), "side", None, None),
            P(("grp", "tok")),
            P("side", "tok"),
            P(),
            P(),
            P(None, ("tok", "side")),
            P(None, ("tok", "side")),
            P(("tok", "side"), None),
            P("grp", None),
        ),
        out_specs=P(("grp", "tok"), None),
        check_vma=False,
    )
```
